32 devices in a mesh: ctx: 16 (over z, y, core), head: 2 (over x).
Axes of the slice: x: 2, y: 2, z: 4, core: 2. Of those that a mesh axis runs over, the one named last changes fastest.
Arguments:
- hidden: bfloat16 [2048, 8192], P('ctx', 'head'), may hold values from -6 to 6
- query: bfloat16 [2048, 8192], P('ctx', 'head'), may hold values from -60 to 60
- fresh_key_value: bfloat16 [2, 2048, 1024], P(None, 'ctx', 'head'), may hold values from -6 to 6
- cached_key_value: bfloat16 [2, 4096, 1024], P(None, 'ctx', 'head'), may hold values from -6 to 6
- positions: int32 [3, 2048], P(None, 'ctx'), may hold values from 0 to 4095
- out_weight: bfloat16 [8192, 8192], P('head', 'ctx'), may hold values from -0.0625 to 0.0625
- norm_gain: float32 [8192], P('head'), may hold values from 0.25 to 1.75
- layer3_key_value_weight: bfloat16 [8192, 2048], P(None, 'head'), may hold values from -0.0625 to 0.0625
- layer3_key_value_bias: float32 [2048], P('head'), may hold values from -3 to 3
- keep_index: int32 [2048], P('ctx'), may hold values from 0 to 127, as said below
- keep_count: int32 [16], P('ctx'), may hold values from 64 to 128, as said below
Outputs:
- layer2_out: bfloat16 [2048, 8192], P('ctx', 'head')
- layer3_packed_key_value: bfloat16 [2048, 2048], P('ctx', 'head')
The draws below stay inside these ranges and needn't reach their ends.
Inputs may be any that keep to these rules, and one draw needn't show every extreme that they name: `keep_index`: within each block of 128 entries, the first keep_count entries are the kept rows in rising order (all text rows and every second visual row), the rest the dropped rows in rising order. `keep_count`: some block keeps all 128 rows in every draw.
All inputs are finite; a program needn't handle non-finite values.
Results may differ from the reference program's by a relative error of at most 0.012.
Values may be sent and summed in bfloat16 or wider, within the bound.
A program may use at most 192 MiB of HBM per device.

```python
import jax
import jax.numpy as jnp
from jax import lax

MODEL_WIDTH = 8192
QUERY_HEADS = 64
KEY_VALUE_HEADS = 8
HEAD_DIMENSION = 128
FRESH_TOKENS = 128
FRESH_TOTAL = 2048
CACHED_TOKENS = 4096


def keep_tables(key):
    block_list = FRESH_TOTAL // FRESH_TOKENS
    first_key, second_key, third_key = jax.random.split(jax.random.fold_in(key, 71), 3)
    visual_share = jax.random.randint(first_key, (block_list, 1), 0, FRESH_TOKENS + 1)
    visual = jax.random.randint(second_key, (block_list, FRESH_TOKENS), 0, FRESH_TOKENS) < visual_share
    chosen_block = jax.random.randint(third_key, (), 0, block_list)
    visual = visual & (jnp.arange(block_list)[:, None] != chosen_block)
    visual_rank = jnp.cumsum(visual.astype(jnp.int32), axis=1) - 1
    dropped = visual & (visual_rank % 2 == 1)
    sort_keys = dropped.astype(jnp.int32) * FRESH_TOKENS + jnp.arange(FRESH_TOKENS, dtype=jnp.int32)[None, :]
    kept_order = jnp.argsort(sort_keys, axis=1, stable=True).astype(jnp.int32)
    kept_count = (FRESH_TOKENS - jnp.sum(dropped.astype(jnp.int32), axis=1)).astype(jnp.int32)
    return (kept_order.reshape(-1), kept_count)


def draw_keep_index(key, part):
    return keep_tables(key)[0]


def draw_keep_count(key, part):
    return keep_tables(key)[1]


def draw_query(key, part):
    first_key = jax.random.fold_in(jax.random.fold_in(key, 13), 0)
    shape = (FRESH_TOTAL, QUERY_HEADS * HEAD_DIMENSION)
    values = jax.random.normal(first_key, shape, jnp.float32)
    return jnp.clip(values, -60.0, 60.0).astype(jnp.bfloat16)


def set_ends(result, key, least, top_value):
    extent = result.shape
    spot = [jax.random.randint(jax.random.fold_in(key, axis), (), 0, extent[axis]) for axis in range(len(extent))]
    result = result.at[tuple(spot)].set(least)
    longest = extent.index(max(extent))
    spot[longest] = (spot[longest] + 1) % extent[longest]
    return result.at[tuple(spot)].set(top_value)


def block_scale(key, shape, pieces, low, high):
    level, own = 1.0, jax.random.fold_in(key, 6)
    for dim, shards_of in pieces:
        steps = jnp.exp(jax.random.uniform(jax.random.fold_in(own, dim), (shards_of,), jnp.float32, low / len(pieces), high / len(pieces)))
        level = level * jnp.repeat(steps, shape[dim] // shards_of).reshape([-1 if axis == dim else 1 for axis in range(len(shape))])
    return level


def normal_values(key, extent, deviation, bound, cuts=(), kind=jnp.bfloat16):
    values = deviation * jax.random.normal(key, extent, jnp.float32)
    if cuts:
        values = values * block_scale(key, extent, cuts, -0.22, 0.18)
    return jnp.clip(values, -bound, bound).astype(kind)


def setup_inputs(seed: int = 0) -> dict:
    streams_of = jax.random.split(jax.random.key(seed), 12)
    return {
        "hidden": normal_values(streams_of[0], (FRESH_TOTAL, MODEL_WIDTH), 1.0, 6.0, ((0, 16), (1, 2))),
        "query": draw_query(jax.random.fold_in(streams_of[11], 71), 0),
        "fresh_key_value": normal_values(streams_of[2], (2, FRESH_TOTAL, KEY_VALUE_HEADS * HEAD_DIMENSION), 1.0, 6.0, ((1, 16), (2, 2))),
        "cached_key_value": normal_values(streams_of[3], (2, CACHED_TOKENS, KEY_VALUE_HEADS * HEAD_DIMENSION), 1.0, 6.0, ((1, 16), (2, 2))),
        "positions": set_ends(jax.random.randint(streams_of[4], (3, FRESH_TOTAL), 0, 4096), jax.random.fold_in(streams_of[4], 1), 0, 4095).astype(jnp.int32),
        "out_weight": normal_values(streams_of[5], (QUERY_HEADS * HEAD_DIMENSION, MODEL_WIDTH), (QUERY_HEADS * HEAD_DIMENSION) ** -0.5, 0.0625, ((0, 2), (1, 16))),
        "norm_gain": jnp.clip(1.0 + 0.15 * jax.random.normal(streams_of[6], (MODEL_WIDTH,), jnp.float32), 0.25, 1.75),
        "layer3_key_value_weight": normal_values(streams_of[7], (MODEL_WIDTH, 2 * KEY_VALUE_HEADS * HEAD_DIMENSION), MODEL_WIDTH ** -0.5, 0.0625, ((1, 2),)),
        "layer3_key_value_bias": normal_values(streams_of[8], (2 * KEY_VALUE_HEADS * HEAD_DIMENSION,), 0.5, 3.0, ((0, 2),), jnp.float32),
        "keep_index": draw_keep_index(jax.random.fold_in(streams_of[11], 71), 0),
        "keep_count": draw_keep_count(jax.random.fold_in(streams_of[11], 71), 0),
    }


def tables(positions, head_size):
    half = head_size // 2
    column = jnp.arange(half)
    frequency = jnp.power(jnp.float32(1000000.0), -(2.0 * column.astype(jnp.float32)) / head_size)
    section = (column >= head_size // 8).astype(jnp.int32) + (column >= head_size // 8 + 3 * head_size // 16).astype(jnp.int32)
    places = positions.astype(jnp.float32)
    chosen = jnp.where(section[None, :] == 0, places[0][:, None], jnp.where(section[None, :] == 1, places[1][:, None], places[2][:, None]))
    angles = chosen * frequency[None, :]
    return (jnp.cos(angles), jnp.sin(angles))

def apply_rotary(x, cosine_table, sine_table):
    half = x.shape[-1] // 2
    first_half = x[..., :half]
    second_half = x[..., half:]
    cosine_table = cosine_table[:, None, :]
    sine_table = sine_table[:, None, :]
    return jnp.concatenate([first_half * cosine_table - second_half * sine_table, second_half * cosine_table + first_half * sine_table], axis=-1)

def reference(hidden, query, fresh_key_value, cached_key_value, positions, out_weight, norm_gain, layer3_key_value_weight, layer3_key_value_bias, keep_index, keep_count):
    fresh_token_count = hidden.shape[0]
    block_list = fresh_token_count // FRESH_TOKENS
    query_group_width = QUERY_HEADS // KEY_VALUE_HEADS
    cosine_table, sine_table = tables(positions, HEAD_DIMENSION)
    rotary_query_rows = apply_rotary(query.astype(jnp.float32).reshape(fresh_token_count, QUERY_HEADS, HEAD_DIMENSION), cosine_table, sine_table).astype(jnp.bfloat16)
    rotary_key_rows = apply_rotary(fresh_key_value[0].astype(jnp.float32).reshape(fresh_token_count, KEY_VALUE_HEADS, HEAD_DIMENSION), cosine_table, sine_table).astype(jnp.bfloat16)
    key_matrix_rows = jnp.concatenate([cached_key_value[0].reshape(CACHED_TOKENS, KEY_VALUE_HEADS, HEAD_DIMENSION), rotary_key_rows], axis=0).transpose(1, 0, 2)
    value_matrix_rows = jnp.concatenate([cached_key_value[1].reshape(CACHED_TOKENS, KEY_VALUE_HEADS, HEAD_DIMENSION), fresh_key_value[1].reshape(fresh_token_count, KEY_VALUE_HEADS, HEAD_DIMENSION)], axis=0).transpose(1, 0, 2)
    grouped_rows = rotary_query_rows.reshape(block_list, FRESH_TOKENS, KEY_VALUE_HEADS, query_group_width, HEAD_DIMENSION).transpose(0, 2, 1, 3, 4)

    def per_block(inputs):
        query_block, block_number = inputs
        query_pos = block_number * FRESH_TOKENS + jnp.arange(FRESH_TOKENS)
        recent = jnp.arange(fresh_token_count)[None, :] <= query_pos[:, None]
        visible = jnp.concatenate([jnp.ones((FRESH_TOKENS, CACHED_TOKENS), bool), recent], axis=1)

        def per_head(head_inputs):
            query_head, key_head, value_head = head_inputs
            scores = jnp.einsum('ngd,ld->ngl', query_head.astype(jnp.float32), key_head.astype(jnp.float32)) * HEAD_DIMENSION ** (-0.5)
            scores = jnp.where(visible[:, None, :], scores, -jnp.inf)
            maxima = lax.optimization_barrier(jnp.max(scores, axis=-1, keepdims=True))
            expos = jnp.exp(scores - maxima)
            totals = lax.optimization_barrier(jnp.sum(expos, axis=-1))
            weights = expos.astype(jnp.bfloat16)
            summed = jnp.einsum('ngl,ld->ngd', weights.astype(jnp.float32), value_head.astype(jnp.float32))
            return summed / totals[..., None]
        return lax.map(per_head, (query_block, key_matrix_rows, value_matrix_rows))
    outputs = lax.map(per_block, (grouped_rows, jnp.arange(block_list)))
    attn = outputs.transpose(0, 2, 1, 3, 4).reshape(fresh_token_count, QUERY_HEADS * HEAD_DIMENSION).astype(jnp.bfloat16)
    projection = jnp.dot(attn, out_weight, preferred_element_type=jnp.float32)
    layer2_out = (hidden.astype(jnp.float32) + projection).astype(jnp.bfloat16)
    widened = layer2_out.astype(jnp.float32)
    mean_square = lax.optimization_barrier(jnp.mean(widened * widened, axis=1))
    normalized_rows = (widened * lax.rsqrt(mean_square + 1e-06)[:, None] * norm_gain).astype(jnp.bfloat16)
    layer_three_key_value = (jnp.dot(normalized_rows, layer3_key_value_weight, preferred_element_type=jnp.float32) + layer3_key_value_bias).reshape(fresh_token_count, KEY_VALUE_HEADS, 2, HEAD_DIMENSION)
    layer_three_keys = apply_rotary(layer_three_key_value[:, :, 0], cosine_table, sine_table)
    layer_three_key_value = jnp.stack([layer_three_keys, layer_three_key_value[:, :, 1]], axis=2).reshape(fresh_token_count, 2 * KEY_VALUE_HEADS * HEAD_DIMENSION).astype(jnp.bfloat16)
    grouped_by_block = layer_three_key_value.reshape(block_list, FRESH_TOKENS, 2 * KEY_VALUE_HEADS * HEAD_DIMENSION)
    indices = keep_index.reshape(block_list, FRESH_TOKENS).astype(jnp.int32)
    selected_rows = jnp.take_along_axis(grouped_by_block, indices[:, :, None], axis=1)
    block_occupied = jnp.arange(FRESH_TOKENS)[None, :] < keep_count[:, None]
    layer3_packed_key_value = jnp.where(block_occupied[:, :, None], selected_rows, jnp.zeros_like(selected_rows)).reshape(fresh_token_count, 2 * KEY_VALUE_HEADS * HEAD_DIMENSION)
    return (layer2_out, layer3_packed_key_value)
```

```python
import functools

import jax
import jax.numpy as jnp
from jax import lax
from jax.experimental import pallas as pl
from jax.experimental.pallas import tpu as pltpu
from jax.sharding import PartitionSpec as P

HEAD_DIMENSION = 128


def tables(positions, head_size):
    half = head_size // 2
    column = jnp.arange(half)
    frequency = jnp.power(jnp.float32(1000000.0), -(2.0 * column.astype(jnp.float32)) / head_size)
    section = (column >= head_size // 8).astype(jnp.int32) + (
        column >= head_size // 8 + 3 * head_size // 16
    ).astype(jnp.int32)
    places = positions.astype(jnp.float32)
    chosen = jnp.where(
        section[None, :] == 0,
        places[0][:, None],
        jnp.where(section[None, :] == 1, places[1][:, None], places[2][:, None]),
    )
    angles = chosen * frequency[None, :]
    return (jnp.cos(angles), jnp.sin(angles))


def apply_rotary(x, cosine_table, sine_table):
    half = x.shape[-1] // 2
    first_half = x[..., :half]
    second_half = x[..., half:]
    cosine_table = cosine_table[:, None, :]
    sine_table = sine_table[:, None, :]
    return jnp.concatenate(
        [
            first_half * cosine_table - second_half * sine_table,
            second_half * cosine_table + first_half * sine_table,
        ],
        axis=-1,
    )


LOG2E = 1.4426950408889634


def attend_kernel(group, causal, last, row_ref, q_ref, k_ref, v_ref, *rest):
    if last:
        m_in, l_in, a_in, out_ref, m_ref, l_ref, a_ref = rest
    else:
        m_out, l_out, a_out, m_ref, l_ref, a_ref = rest
    step = pl.program_id(1)
    head = k_ref.shape[1]
    rows = q_ref.shape[0]
    block = k_ref.shape[0]

    @pl.when(step == 0)
    def _():
        if last:
            m_ref[...] = m_in[0]
            l_ref[...] = l_in[0]
            a_ref[...] = a_in[0]
        else:
            m_ref[...] = jnp.full_like(m_ref, -1e30)
            l_ref[...] = jnp.zeros_like(l_ref)
            a_ref[...] = jnp.zeros_like(a_ref)

    def update(masked):
        key = k_ref[...]
        value = v_ref[...]
        scale = LOG2E * head ** (-0.5)
        if masked:
            key_pos = step * block + lax.broadcasted_iota(jnp.int32, (rows, block), 1)
            query_pos = row_ref[0] + lax.broadcasted_iota(jnp.int32, (rows, block), 0)
            visible = key_pos <= query_pos
        for g in range(group):
            part = pl.ds(g * rows, rows)
            s = lax.dot_general(
                q_ref[:, g * head : (g + 1) * head],
                key,
                (((1,), (1,)), ((), ())),
                preferred_element_type=jnp.float32,
            )
            if masked:
                s = jnp.where(visible, s, -1e30)
            old = m_ref[part, :]
            new = jnp.maximum(old, jnp.max(s, axis=1, keepdims=True))
            m_ref[part, :] = new
            e = jnp.exp2((s - new[:, :1]) * scale)
            factor = jnp.exp2((old - new) * scale)
            l_ref[part, :] = l_ref[part, :] * factor + jnp.sum(e, axis=1, keepdims=True)
            a_ref[part, :] = a_ref[part, :] * factor + jnp.dot(
                e.astype(jnp.bfloat16), value, preferred_element_type=jnp.float32
            )

    if causal:
        start = step * block

        @pl.when(start + block - 1 <= row_ref[0])
        def _():
            update(False)

        @pl.when((start + block - 1 > row_ref[0]) & (start <= row_ref[0] + rows - 1))
        def _():
            update(True)
    else:
        update(False)

    @pl.when(step == pl.num_programs(1) - 1)
    def _():
        if last:
            for g in range(group):
                part = pl.ds(g * rows, rows)
                out_ref[:, g * head : (g + 1) * head] = (
                    a_ref[part, :] / l_ref[part, :]
                ).astype(out_ref.dtype)
        else:
            m_out[0] = m_ref[...]
            l_out[0] = l_ref[...]
            a_out[0] = a_ref[...]


def attend(query, key_value, first_row, state, head_size):
    rows, width = query.shape
    length = key_value.shape[1]
    kv_local = key_value.shape[2] // head_size
    group = width // head_size // kv_local
    block = 1024
    while length % block:
        block //= 2
    last = state is not None
    high = group * rows
    carry = pl.BlockSpec((1, high, head_size), lambda k, i, r: (k, 0, 0))
    carry_shape = jax.ShapeDtypeStruct((kv_local, high, head_size), jnp.float32)
    wide = pl.BlockSpec((rows, group * head_size), lambda k, i, r: (0, k))
    in_specs = [
        wide,
        pl.BlockSpec((None, block, head_size), lambda k, i, r: (0, i, k)),
        pl.BlockSpec((None, block, head_size), lambda k, i, r: (1, i, k)),
    ] + ([carry] * 3 if last else [])
    operands = (query, key_value, key_value) + (state if last else ())
    return pl.pallas_call(
        functools.partial(attend_kernel, group, last, last),
        out_shape=jax.ShapeDtypeStruct((rows, width), jnp.bfloat16) if last else (carry_shape,) * 3,
        grid_spec=pltpu.PrefetchScalarGridSpec(
            num_scalar_prefetch=1,
            grid=(kv_local, length // block),
            in_specs=in_specs,
            out_specs=wide if last else (carry,) * 3,
            scratch_shapes=[pltpu.VMEM((high, head_size), jnp.float32)] * 3,
        ),
        compiler_params=pltpu.CompilerParams(vmem_limit_bytes=40 * 1024 * 1024),
        cost_estimate=pl.CostEstimate(
            flops=8 * rows * width * length,
            bytes_accessed=4 * length * kv_local * head_size + 4 * rows * width,
            transcendentals=rows * (width // head_size) * length,
        ),
    )(first_row.reshape(1), *operands)


def scatter_kernel(chips, cores, heads, x_ref, o_ref, send_sem, recv_sem, tile, local_sem):
    me = lax.axis_index("ctx")
    h = lax.axis_index("head")
    chip = me // cores
    core = me % cores
    per = chips // heads
    owner_head = chip // per
    slot = h * per + chip % per
    barrier = pltpu.get_barrier_semaphore()
    for d in range(chips):
        there = lax.rem(chip + d, chips) * cores + core
        for e in range(heads):
            if d or e:
                pl.semaphore_signal(
                    barrier,
                    inc=1,
                    device_id=(there, lax.rem(h + e, heads)),
                    device_id_type=pl.DeviceIdType.MESH,
                )
    pl.semaphore_wait(barrier, chips * heads - 1)

    def copy_to(d):
        p = lax.rem(chip + d, chips)
        return pltpu.make_async_remote_copy(
            src_ref=x_ref.at[p],
            dst_ref=o_ref.at[slot],
            send_sem=send_sem.at[d],
            recv_sem=recv_sem.at[slot],
            device_id=(p * cores + core, owner_head),
            device_id_type=pl.DeviceIdType.MESH,
        )

    def receive(s):
        return pltpu.make_async_remote_copy(
            src_ref=x_ref.at[0],
            dst_ref=o_ref.at[s],
            send_sem=send_sem.at[0],
            recv_sem=recv_sem.at[s],
            device_id=(me, lax.rem(h + 1, heads)),
            device_id_type=pl.DeviceIdType.MESH,
        )

    for d in range(1, chips):
        copy_to(d).start()

    @pl.when(owner_head != h)
    def _():
        copy_to(0).start()

    @pl.when(owner_head == h)
    def _():
        into = pltpu.make_async_copy(x_ref.at[chip], tile, local_sem.at[0])
        into.start()
        into.wait()
        out = pltpu.make_async_copy(tile, o_ref.at[slot], local_sem.at[1])
        out.start()
        out.wait()

    for d in range(1, chips):
        copy_to(d).wait_send()

    @pl.when(owner_head != h)
    def _():
        copy_to(0).wait_send()

    for s in range(chips):

        @pl.when(jnp.logical_or(owner_head != h, slot != s))
        def _():
            receive(s).wait_recv()


def scatter_columns(product, chips, cores, heads):
    block = product.shape[1:]
    moved = pl.pallas_call(
        functools.partial(scatter_kernel, chips, cores, heads),
        out_shape=jax.ShapeDtypeStruct(product.shape, product.dtype),
        in_specs=[pl.BlockSpec(memory_space=pl.ANY)],
        out_specs=pl.BlockSpec(memory_space=pl.ANY),
        scratch_shapes=[
            pltpu.SemaphoreType.DMA((chips,)),
            pltpu.SemaphoreType.DMA((chips,)),
            pltpu.VMEM(block, product.dtype),
            pltpu.SemaphoreType.DMA((2,)),
        ],
        compiler_params=pltpu.CompilerParams(collective_id=0, has_side_effects=True),
    )(product)
    return moved.reshape((heads, chips // heads) + block)


def gather_kernel(depth, cores, x_ref, o_ref, send_sem, recv_sem, tile, local_sem):
    me = lax.axis_index("ctx")
    h = lax.axis_index("head")
    chip = me // cores
    core = me % cores
    ring = chip // 2
    side = chip % 2
    pair = ring * 2 + (1 - side)

    def along(d):
        return lax.rem(ring + d, depth)

    barrier = pltpu.get_barrier_semaphore()
    for d in range(1, depth):
        pl.semaphore_signal(
            barrier,
            inc=1,
            device_id=((along(d) * 2 + side) * cores + core, h),
            device_id_type=pl.DeviceIdType.MESH,
        )
    pl.semaphore_signal(
        barrier, inc=1, device_id=(pair * cores + core, h), device_id_type=pl.DeviceIdType.MESH
    )
    pl.semaphore_wait(barrier, depth)

    def send(source, half, origin, target, kind, d):
        return pltpu.make_async_remote_copy(
            src_ref=source,
            dst_ref=o_ref.at[origin, half],
            send_sem=send_sem.at[kind, d],
            recv_sem=recv_sem.at[half, origin],
            device_id=(target * cores + core, h),
            device_id_type=pl.DeviceIdType.MESH,
        )

    def receive(half, origin):
        send(x_ref.at[half], half, origin, pair, 0, 0).wait_recv()

    sent = [send(x_ref.at[0], 0, chip, pair, 0, 0), send(x_ref.at[1], 1, chip, pair, 1, 0)]
    order = [d for pair_of in zip(range(1, depth), range(depth - 1, 0, -1)) for d in pair_of]
    order = list(dict.fromkeys(order))
    for d in order:
        sent.append(send(x_ref.at[1], 1, chip, along(d) * 2 + side, 2, d))
    for d in order:
        sent.append(send(x_ref.at[0], 0, chip, along(d) * 2 + side, 3, d))
    for copy in sent:
        copy.start()
    into = pltpu.make_async_copy(x_ref, tile, local_sem.at[0])
    into.start()
    into.wait()
    out = pltpu.make_async_copy(tile, o_ref.at[chip], local_sem.at[1])
    out.start()

    receive(0, pair)
    for d in order:
        copy = send(o_ref.at[pair, 0], 0, pair, along(d) * 2 + side, 4, d)
        copy.start()
        sent.append(copy)
    for d in order:
        origin = along(d) * 2 + side
        receive(1, origin)
        copy = send(o_ref.at[origin, 1], 1, origin, pair, 1, d)
        copy.start()
        sent.append(copy)
    for d in range(1, depth):
        receive(0, along(d) * 2 + side)
    receive(1, pair)
    for d in range(1, depth):
        receive(0, along(d) * 2 + 1 - side)
        receive(1, along(d) * 2 + 1 - side)
    for copy in sent:
        copy.wait_send()
    out.wait()


def gather_rows(x, chips, cores):
    rows, width = x.shape
    halves = x.reshape(2, rows // 2, width)
    return pl.pallas_call(
        functools.partial(gather_kernel, chips // 2, cores),
        out_shape=jax.ShapeDtypeStruct((chips,) + halves.shape, x.dtype),
        in_specs=[pl.BlockSpec(memory_space=pl.ANY)],
        out_specs=pl.BlockSpec(memory_space=pl.ANY),
        scratch_shapes=[
            pltpu.SemaphoreType.DMA((5, chips // 2)),
            pltpu.SemaphoreType.DMA((2, chips)),
            pltpu.VMEM(halves.shape, x.dtype),
            pltpu.SemaphoreType.DMA((2,)),
        ],
        compiler_params=pltpu.CompilerParams(collective_id=1, has_side_effects=True),
    )(halves).reshape(chips * rows, width)


MESH = pl.DeviceIdType.MESH


def fused_kernel(depth, group, heads, key_block, *refs):
    (cos_ref, sin_ref, q_ref, fresh_ref, cached_ref, w_ref, hidden_ref, out_ref,
     qrot, qall, frot, kc, kf, s_ref, av, st, wv, acc_ref, cst, crecv,
     kvs, kvr, kys, kcs, loc, qs, qr, ws, wr, wos, wor, wfs, wfr,
     xs, xr, us, ds, ys, zr, yr, cs, cr) = refs
    rows = q_ref.shape[0]
    head_size = kc.shape[2]
    half = rows // heads
    cached_rows = cached_ref.shape[1]
    chips = depth * 2
    per = chips // heads
    me = lax.axis_index("ctx")
    h = lax.axis_index("head")
    chip = me // 2
    c = me % 2
    z = chip // 2
    y = chip % 2
    pair_blocks = group // 2
    pieces = 4 * depth
    early = depth
    piece = w_ref.shape[0] // pieces
    width = w_ref.shape[1]

    def ctx(zz, yy, cc):
        return (zz * 2 + yy) * 2 + cc

    def remote(src, dst, ssem, rsem, zz, yy, cc, hh):
        return pltpu.make_async_remote_copy(
            src_ref=src, dst_ref=dst, send_sem=ssem, recv_sem=rsem,
            device_id=(ctx(zz, yy, cc), hh), device_id_type=MESH,
        )

    def order(i):
        return i + 1 - 2 * (i % 2)

    own_w = pltpu.make_async_copy(w_ref, wv.at[h, c], loc.at[0])
    own_w.start()

    def lanes(index):
        return pl.ds(pl.multiple_of(index * head_size, head_size), head_size)

    def slot(kind, zz, yy, cc):
        where = ctx(zz, yy, cc)
        if kind == 0:
            return kc.at[:, pl.ds(pl.multiple_of(where * cached_rows, cached_rows), cached_rows), :]
        return kf.at[:, pl.ds(pl.multiple_of(where * rows, rows), rows), :]

    own_c = pltpu.make_async_copy(cached_ref.at[:, :, lanes(z)], slot(0, z, y, c), loc.at[1])
    own_c.start()

    cosine = cos_ref[...]
    sine = sin_ref[...]

    def rotate(x):
        x = x.astype(jnp.float32)
        return (x * cosine + pltpu.roll(x, head_size // 2, 1) * sine).astype(jnp.bfloat16)

    for g in range(depth):
        part = slice(g * head_size, (g + 1) * head_size)
        frot[g, 0] = rotate(fresh_ref[0, :, part])
        frot[g, 1] = fresh_ref[1, :, part]
    for j in range(depth * group):
        part = slice(j * head_size, (j + 1) * head_size)
        qrot[j // group, j % group] = rotate(q_ref[:, part])
    qall[z] = qrot[z]
    own_f = pltpu.make_async_copy(frot.at[z], slot(1, z, y, c), loc.at[2])
    own_f.start()

    barrier = pltpu.get_barrier_semaphore()
    for d in range(chips):
        for e in range(heads):
            if d or e:
                pl.semaphore_signal(
                    barrier, inc=1,
                    device_id=(lax.rem(chip + d, chips) * 2 + c, lax.rem(h + e, heads)),
                    device_id_type=MESH,
                )
    pl.semaphore_signal(barrier, inc=1, device_id=(ctx(z, y, 1 - c), h), device_id_type=MESH)
    pl.semaphore_wait(barrier, chips * heads)

    def kv_send(d, kind):
        to = lax.rem(z + d, depth)
        src = cached_ref.at[:, :, lanes(to)] if kind == 0 else frot.at[to]
        return remote(
            src, slot(kind, z, y, c), kvs.at[d, kind], kvr.at[kind, ctx(z, y, c)], to, y, c, h
        )

    def kv_pair(zz, kind):
        where = slot(kind, zz, y, c)
        return remote(where, where, kys.at[zz, kind], kvr.at[kind, ctx(zz, y, c)], z, 1 - y, c, h)

    def kv_core(zz, yy, kind):
        where = slot(kind, zz, yy, c)
        return remote(
            where, where, kcs.at[zz * 2 + yy, kind], kvr.at[kind, ctx(zz, yy, c)], z, y, 1 - c, h
        )

    def kv_landed(zz, yy, cc, kind):
        where = slot(kind, zz, yy, cc)
        remote(
            where, where, kcs.at[0, 0], kvr.at[kind, ctx(zz, yy, cc)], z, 1 - y, c, h
        ).wait_recv()

    def q_send(d):
        to = lax.rem(z + d, depth)
        return remote(qrot.at[to], qall.at[z], qs.at[d], qr.at[z], to, y, c, h)

    def w_send(k):
        part = pl.ds(pl.multiple_of(k * piece, piece), piece)
        return remote(
            w_ref.at[part, :], wv.at[h, c, part, :], ws.at[k], wr.at[k], z, y, c, 1 - h
        )

    def w_forward(k):
        part = pl.ds(pl.multiple_of(k * piece, piece), piece)
        where = wv.at[1 - h, c, part, :]
        return remote(where, where, wfs.at[k], wfr.at[k], z, y, 1 - c, h)

    def w_landed(k):
        part = pl.ds(pl.multiple_of(k * piece, piece), piece)
        where = wv.at[1 - h, c, part, :]
        remote(where, where, wfs.at[k], wr.at[k], z, y, c, 1 - h).wait_recv()

    def w_forwarded(k):
        part = pl.ds(pl.multiple_of(k * piece, piece), piece)
        where = wv.at[1 - h, 1 - c, part, :]
        remote(where, where, wfs.at[k], wfr.at[k], z, y, 1 - c, h).wait_recv()

    own_w_core = remote(w_ref, wv.at[h, c], wos.at[0], wor.at[0], z, y, 1 - c, h)

    first = order(0)
    for d in range(1, depth):
        for kind in range(2):
            kv_send(d, kind).start()
    for k in range(early):
        w_send(k).start()

    @pl.when(z == first)
    def _():
        for d in range(1, depth):
            q_send(d).start()

    own_c.wait()
    own_f.wait()
    for kind in range(2):
        kv_pair(z, kind).start()
        kv_core(z, y, kind).start()
    for s in range(1, depth):
        for sign in (-1, 1):
            zz = z + sign * s

            @pl.when((zz >= 0) & (zz < depth))
            def _():
                for kind in range(2):
                    kv_landed(zz, y, c, kind)
                    kv_pair(zz, kind).start()
                    kv_core(zz, y, kind).start()

    @pl.when(z != first)
    def _():
        for d in range(1, depth):
            q_send(d).start()

    for zz in range(depth):
        for kind in range(2):
            kv_landed(zz, 1 - y, c, kind)
            kv_core(zz, 1 - y, kind).start()
    for zz in range(depth):
        for yy in range(2):
            for kind in range(2):
                kv_landed(zz, yy, 1 - c, kind)
    own_w_core.start()

    def x_send(e):
        zp = order(e)
        return remote(st.at[e], av.at[zp, h, z, y], xs.at[e], xr.at[e], z, y, c, 1 - h)

    def x_landed(e):
        zp = order(e)
        remote(st.at[e], av.at[zp, 1 - h, z, y], xs.at[e], xr.at[e], z, y, c, 1 - h).wait_recv()

    def up(e, zz):
        where = av.at[order(e), :, zz, y]
        return remote(where, where, us.at[e, zz], zr.at[e, zz], z + 1, y, c, h)

    def down(e, zz):
        where = av.at[order(e), :, zz, y]
        return remote(where, where, ds.at[e, zz], zr.at[e, zz], z - 1, y, c, h)

    def across(e, zz):
        where = av.at[order(e), :, zz, y]
        return remote(where, where, ys.at[e, zz], yr.at[e, zz], z, 1 - y, c, h)

    def own_out(e):
        x_landed(e)

        @pl.when(z + 1 < depth)
        def _():
            up(e, z).start()

        @pl.when(z >= 1)
        def _():
            down(e, z).start()

        across(e, z).start()

    def chain_landed(e, zz):
        where = av.at[order(e), :, zz, y]
        remote(where, where, ys.at[e, zz], zr.at[e, zz], z, 1 - y, c, h).wait_recv()

    def hop(e, s):
        @pl.when(z >= s)
        def _():
            chain_landed(e, z - s)

            @pl.when(z + 1 < depth)
            def _():
                up(e, z - s).start()

            across(e, z - s).start()

        @pl.when(z + s < depth)
        def _():
            chain_landed(e, z + s)

            @pl.when(z >= 1)
            def _():
                down(e, z + s).start()

            across(e, z + s).start()

    def across_landed(e):
        for zz in range(depth):
            where = av.at[order(e), :, zz, 1 - y]
            remote(where, where, ys.at[e, zz], yr.at[e, zz], z, 1 - y, c, h).wait_recv()

    scale = LOG2E * head_size ** (-0.5)
    both = 2 * rows
    lane_groups = key_block // head_size
    cached_blocks = kc.shape[1] // key_block

    def attend_pair(i, p):
        zp = order(i)
        q = qall[zp, pl.ds(2 * p, 2)].reshape(both, head_size)
        block = ctx(zp, y, c)
        fresh_blocks = (block * rows + rows + key_block - 1) // key_block

        def scores(keys):
            return lax.dot_general(
                q, keys, (((1,), (1,)), ((), ())), preferred_element_type=jnp.float32
            )

        def widen(s, top):
            for u in range(lane_groups):
                top = jnp.maximum(top, s[:, u * head_size : (u + 1) * head_size])
            return top

        top = jnp.full((both, head_size), -1e30, jnp.float32)
        for b in range(cached_blocks):
            s = scores(kc[0, b * key_block : (b + 1) * key_block, :])
            s_ref[b] = s
            top = widen(s, top)

        def fresh_scores(b, top):
            keys = kf[0, pl.ds(pl.multiple_of(b * key_block, key_block), key_block), :]
            s = scores(keys)
            key_pos = b * key_block + lax.broadcasted_iota(jnp.int32, (rows, key_block), 1)
            query_pos = block * rows + lax.broadcasted_iota(jnp.int32, (rows, key_block), 0)
            visible = key_pos <= query_pos
            s = jnp.where(jnp.concatenate([visible, visible], axis=0), s, -1e30)
            s_ref[cached_blocks + b] = s
            return widen(s, top)

        top = lax.fori_loop(0, fresh_blocks, fresh_scores, top)
        peak = jnp.max(top, axis=1, keepdims=True)

        def weigh(s, values, total, summed):
            e = jnp.exp2((s - peak) * scale)
            for u in range(lane_groups):
                total = total + e[:, u * head_size : (u + 1) * head_size]
            summed = summed + jnp.dot(
                e.astype(jnp.bfloat16), values, preferred_element_type=jnp.float32
            )
            return total, summed

        total = jnp.zeros((both, head_size), jnp.float32)
        summed = jnp.zeros((both, head_size), jnp.float32)
        for b in range(cached_blocks):
            total, summed = weigh(
                s_ref[b], kc[1, b * key_block : (b + 1) * key_block, :], total, summed
            )

        def fresh_weigh(b, carry):
            values = kf[1, pl.ds(pl.multiple_of(b * key_block, key_block), key_block), :]
            return weigh(s_ref[cached_blocks + b], values, *carry)

        total, summed = lax.fori_loop(0, fresh_blocks, fresh_weigh, (total, summed))
        out = (summed / jnp.sum(total, axis=1, keepdims=True)).astype(jnp.bfloat16)
        for a in range(2):
            upper = out[a * rows : a * rows + half]
            lower = out[a * rows + half : (a + 1) * rows]
            where = pl.ds(pl.multiple_of((2 * p + a) * head_size, head_size), head_size)
            av[zp, h, z, y, :, where] = jnp.where(h == 0, upper, lower)
            st[i, :, where] = jnp.where(h == 0, lower, upper)

    def step(t, carry):
        i = t // pair_blocks
        p = t % pair_blocks

        @pl.when((p == 0) & (order(i) != z))
        def _():
            zp = order(i)
            remote(qrot.at[0], qall.at[zp], qs.at[0], qr.at[zp], z, 1 - y, c, h).wait_recv()

        attend_pair(i, p)

        @pl.when((p == 0) & (i >= 1))
        def _():
            x_send(i - 1).start()

        @pl.when(p >= 1)
        def _():
            w_send(early + 3 * i + p - 1).start()

        @pl.when((p == 1) & (i >= 1))
        def _():
            own_out(i - 1)
            low = jnp.where(i == 1, 0, early + 3 * (i - 2))

            def forward(k, carry):
                w_landed(k)
                w_forward(k).start()
                return carry

            lax.fori_loop(low, early + 3 * (i - 1), forward, 0)

        @pl.when((p == 3) & (i >= 1))
        def _():
            hop(i - 1, 1)

        if depth > 2:
            @pl.when((p == 1) & (i >= 2))
            def _():
                hop(i - 2, 2)

            @pl.when((p == 3) & (i >= 2))
            def _():
                for s in range(3, depth):
                    hop(i - 2, s)

        return carry

    lax.fori_loop(0, depth * pair_blocks, step, 0)

    owner = chip // per
    place = chip % per

    def tile_send(e, yy):
        zp = order(e)
        return remote(
            cst.at[e, yy], crecv.at[h, place], cs.at[e, yy], cr.at[h, place], zp, yy, c, owner
        )

    def is_self(e, yy):
        return (order(e) == z) & (y == yy) & (owner == h)

    def project(e):
        zp = order(e)
        across_landed(e)
        acc_ref[...] = jnp.zeros_like(acc_ref)
        span = av.shape[5]

        def term(k, carry):
            xx = k // depth
            zz = k % depth
            left = av[zp, xx, zz].reshape(2 * half, span)
            for cc in range(2):
                part = pl.ds(cc * width, width)
                acc_ref[:, part] += jnp.dot(
                    left,
                    wv[xx, cc, pl.ds(pl.multiple_of(zz * span, span), span), :],
                    preferred_element_type=jnp.float32,
                )
            return carry

        lax.fori_loop(0, heads * depth, term, 0)
        for yy in range(2):
            cst[e, yy] = acc_ref[yy * half : (yy + 1) * half, :].astype(jnp.bfloat16)

        for yy in range(2):
            @pl.when(is_self(e, yy))
            def _():
                crecv[h, place] = cst[e, yy]

            @pl.when(jnp.logical_not(is_self(e, yy)))
            def _():
                tile_send(e, yy).start()

    last = depth - 1
    x_send(last).start()
    if depth > 2:
        hop(last - 1, 2)
    own_out(last)
    for s in range(3, depth):
        hop(last - 1, s)

    def forward(k, carry):
        w_landed(k)
        w_forward(k).start()
        return carry

    hop(last, 1)
    lax.fori_loop(early + 3 * (depth - 2), pieces, forward, 0)
    own_w.wait()
    remote(w_ref, wv.at[h, 1 - c], wos.at[0], wor.at[0], z, y, 1 - c, h).wait_recv()

    def forwarded(k, carry):
        w_forwarded(k)
        return carry

    lax.fori_loop(0, pieces, forwarded, 0)
    for e in range(depth):
        if e + 2 < depth:
            project(e)
            hop(last, e + 2)
        else:
            project(e)

    for xx in range(heads):
        for s in range(per):
            @pl.when(jnp.logical_not((h * per + s == chip) & (h == xx)))
            def _():
                remote(
                    cst.at[0, 0], crecv.at[xx, s], cs.at[0, 0], cr.at[xx, s], z, 1 - y, c, h
                ).wait_recv()

            rows_of = slice(xx * half, (xx + 1) * half)
            columns = slice(s * 2 * width, (s + 1) * 2 * width)
            out_ref[rows_of, columns] = (
                hidden_ref[rows_of, columns].astype(jnp.float32)
                + crecv[xx, s].astype(jnp.float32)
            ).astype(jnp.bfloat16)

    for d in range(1, depth):
        for kind in range(2):
            kv_send(d, kind).wait_send()
        q_send(d).wait_send()
    for zz in range(depth):
        for kind in range(2):
            kv_pair(zz, kind).wait_send()
            for yy in range(2):
                kv_core(zz, yy, kind).wait_send()
    own_w_core.wait_send()

    def w_sent(k, carry):
        w_send(k).wait_send()
        w_forward(k).wait_send()
        return carry

    lax.fori_loop(0, pieces, w_sent, 0)
    for e in range(depth):
        x_send(e).wait_send()
        for zz in range(depth):
            across(e, zz).wait_send()

            @pl.when((zz <= z) & (z + 1 < depth))
            def _():
                up(e, zz).wait_send()

            @pl.when((zz >= z) & (z >= 1))
            def _():
                down(e, zz).wait_send()

        for yy in range(2):
            @pl.when(jnp.logical_not(is_self(e, yy)))
            def _():
                tile_send(e, yy).wait_send()


def fused(cosine, sine, query, fresh, cached, weight, hidden, depth, heads):
    rows, wide = query.shape
    head_size = HEAD_DIMENSION
    group = wide // head_size // depth
    contexts = depth * 4
    half = rows // heads
    key_block = 512
    cached_total = contexts * cached.shape[1]
    fresh_total = contexts * rows
    while cached_total % key_block or fresh_total % key_block:
        key_block //= 2
    pieces = 4 * depth
    per = depth * 2 // heads
    dma = pltpu.SemaphoreType.DMA
    bf16 = jnp.bfloat16
    vmem = pltpu.VMEM
    whole = pl.BlockSpec(memory_space=pltpu.VMEM)
    far = pl.BlockSpec(memory_space=pl.ANY)
    return pl.pallas_call(
        functools.partial(fused_kernel, depth, group, heads, key_block),
        out_shape=jax.ShapeDtypeStruct(hidden.shape, bf16),
        in_specs=[whole, whole, whole, whole, far, far, whole],
        out_specs=whole,
        scratch_shapes=[
            vmem((depth, group, rows, head_size), bf16),
            vmem((depth, group, rows, head_size), bf16),
            vmem((depth, 2, rows, head_size), bf16),
            vmem((2, cached_total, head_size), bf16),
            vmem((2, fresh_total, head_size), bf16),
            vmem(((cached_total + fresh_total) // key_block, 2 * rows, key_block), jnp.float32),
            vmem((depth, heads, depth, 2, half, group * head_size), bf16),
            vmem((depth, half, group * head_size), bf16),
            vmem((heads, 2) + weight.shape, bf16),
            vmem((rows, 2 * weight.shape[1]), jnp.float32),
            vmem((depth, 2, half, 2 * weight.shape[1]), bf16),
            vmem((heads, per, half, 2 * weight.shape[1]), bf16),
            dma((depth, 2)), dma((2, contexts)), dma((depth, 2)), dma((depth * 2, 2)),
            dma((3,)), dma((depth,)), dma((depth,)),
            dma((pieces,)), dma((pieces,)), dma((1,)), dma((1,)), dma((pieces,)), dma((pieces,)),
            dma((depth,)), dma((depth,)),
            dma((depth, depth)), dma((depth, depth)), dma((depth, depth)),
            dma((depth, depth)), dma((depth, depth)),
            dma((depth, 2)), dma((heads, per)),
        ],
        compiler_params=pltpu.CompilerParams(
            collective_id=2, has_side_effects=True, vmem_limit_bytes=60 * 1024 * 1024
        ),
    )(cosine, sine, query, fresh, cached, weight, hidden)


def exchange(x, axis_name, size):
    return lax.ppermute(x, axis_name, [(i, i ^ 1) for i in range(size)])


def local(
    contexts,
    heads,
    hidden,
    query,
    fresh_key_value,
    cached_key_value,
    positions,
    out_weight,
    norm_gain,
    layer3_key_value_weight,
    layer3_key_value_bias,
    keep_index,
    keep_count,
):
    new_rows = hidden.shape[0]
    head_size = HEAD_DIMENSION
    kv_local = fresh_key_value.shape[2] // head_size
    q_local = query.shape[1] // head_size
    cores = 2
    chips = contexts // cores
    me = lax.axis_index("ctx")
    core = me % cores
    head = lax.axis_index("head")
    cosine_table, sine_table = tables(positions, head_size)
    if heads == 2:
        other_gain = exchange(norm_gain, "head", heads)
        whole_gain = jnp.concatenate(
            [jnp.where(head == 0, norm_gain, other_gain), jnp.where(head == 0, other_gain, norm_gain)]
        )
    else:
        whole_gain = lax.all_gather(norm_gain, "head", axis=0, tiled=True)
    if heads == 2 and kv_local * 2 == chips and q_local == 8 * kv_local:
        layer2_out = fused(
            jnp.concatenate([cosine_table, cosine_table], axis=1),
            jnp.concatenate([-sine_table, sine_table], axis=1),
            query,
            fresh_key_value,
            cached_key_value,
            out_weight,
            hidden,
            kv_local,
            heads,
        )
    else:
        rotary_query_rows = apply_rotary(
            query.astype(jnp.float32).reshape(new_rows, q_local, head_size), cosine_table, sine_table
        ).astype(jnp.bfloat16).reshape(new_rows, q_local * head_size)
        rotary_key_rows = apply_rotary(
            fresh_key_value[0].astype(jnp.float32).reshape(new_rows, kv_local, head_size),
            cosine_table,
            sine_table,
        ).astype(jnp.bfloat16)
        recent = jnp.stack(
            [rotary_key_rows.reshape(new_rows, kv_local * head_size), fresh_key_value[1]]
        )
        other_weight = exchange(out_weight, "ctx", contexts)
        first_row = me * new_rows
        cached_all = lax.all_gather(cached_key_value, "ctx", axis=1, tiled=True)
        recent_all = lax.all_gather(recent, "ctx", axis=1, tiled=True)
        state = attend(rotary_query_rows, cached_all, first_row, None, head_size)
        attn = attend(rotary_query_rows, recent_all, first_row, tuple(state), head_size)
        outputs = gather_rows(attn, chips, cores)
        own = jnp.dot(outputs, out_weight, preferred_element_type=jnp.float32).astype(jnp.bfloat16)
        other = jnp.dot(outputs, other_weight, preferred_element_type=jnp.float32).astype(jnp.bfloat16)
        product = jnp.concatenate(
            [jnp.where(core == 0, own, other), jnp.where(core == 0, other, own)], axis=1
        ).reshape(chips, new_rows, -1)
        parts = scatter_columns(product, chips, cores, heads)
        head_summed = jnp.sum(parts.astype(jnp.float32), axis=0)
        head_summed = head_summed.transpose(1, 0, 2).reshape(hidden.shape)
        layer2_out = (hidden.astype(jnp.float32) + head_summed).astype(jnp.bfloat16)
    if heads == 2:
        other_out = exchange(layer2_out, "head", heads)
        whole_out = jnp.concatenate(
            [
                jnp.where(head == 0, layer2_out, other_out),
                jnp.where(head == 0, other_out, layer2_out),
            ],
            axis=1,
        )
    else:
        whole_out = lax.all_gather(layer2_out, "head", axis=1, tiled=True)
    widened = whole_out.astype(jnp.float32)
    squares = jnp.sum(widened * widened, axis=1)
    level = lax.rsqrt(squares / widened.shape[1] + 1e-06)[:, None]
    full_rows = (widened * level * whole_gain).astype(jnp.bfloat16)
    full_rows = lax.optimization_barrier(full_rows)
    layer_three_key_value = (
        jnp.dot(full_rows, layer3_key_value_weight, preferred_element_type=jnp.float32)
        + layer3_key_value_bias
    ).reshape(new_rows, kv_local, 2, head_size)
    layer_three_keys = apply_rotary(layer_three_key_value[:, :, 0], cosine_table, sine_table)
    layer_three_key_value = (
        jnp.stack([layer_three_keys, layer_three_key_value[:, :, 1]], axis=2)
        .reshape(new_rows, 2 * kv_local * head_size)
        .astype(jnp.bfloat16)
    )
    selected_rows = jnp.take(layer_three_key_value, keep_index, axis=0)
    block_occupied = jnp.arange(new_rows) < keep_count[0]
    layer3_packed_key_value = jnp.where(
        block_occupied[:, None], selected_rows, jnp.zeros_like(selected_rows)
    )
    return (layer2_out, layer3_packed_key_value)


def solution(mesh):
    placed = (
        P("ctx", "head"),
        P("ctx", "head"),
        P(None, "ctx", "head"),
        P(None, "ctx", "head"),
        P(None, "ctx"),
        P("head", "ctx"),
        P("head"),
        P(None, "head"),
        P("head"),
        P("ctx"),
        P("ctx"),
    )
    return jax.shard_map(
        functools.partial(local, mesh.shape["ctx"], mesh.shape["head"]),
        mesh=mesh,
        in_specs=placed,
        out_specs=(P("ctx", "head"), P("ctx", "head")),
        check_vma=False,
    )
```

```python
import functools

import jax
import jax.numpy as jnp
from jax import lax
from jax.experimental import pallas as pl
from jax.experimental.pallas import tpu as pltpu
from jax.sharding import PartitionSpec as P

HEAD_DIMENSION = 128


def tables(positions, head_size):
    half = head_size // 2
    column = jnp.arange(half)
    frequency = jnp.power(jnp.float32(1000000.0), -(2.0 * column.astype(jnp.float32)) / head_size)
    section = (column >= head_size // 8).astype(jnp.int32) + (
        column >= head_size // 8 + 3 * head_size // 16
    ).astype(jnp.int32)
    places = positions.astype(jnp.float32)
    chosen = jnp.where(
        section[None, :] == 0,
        places[0][:, None],
        jnp.where(section[None, :] == 1, places[1][:, None], places[2][:, None]),
    )
    angles = chosen * frequency[None, :]
    return (jnp.cos(angles), jnp.sin(angles))


def apply_rotary(x, cosine_table, sine_table):
    half = x.shape[-1] // 2
    first_half = x[..., :half]
    second_half = x[..., half:]
    cosine_table = cosine_table[:, None, :]
    sine_table = sine_table[:, None, :]
    return jnp.concatenate(
        [
            first_half * cosine_table - second_half * sine_table,
            second_half * cosine_table + first_half * sine_table,
        ],
        axis=-1,
    )


LOG2E = 1.4426950408889634


def attend_kernel(group, causal, last, row_ref, q_ref, k_ref, v_ref, *rest):
    if last:
        m_in, l_in, a_in, out_ref, m_ref, l_ref, a_ref = rest
    else:
        m_out, l_out, a_out, m_ref, l_ref, a_ref = rest
    step = pl.program_id(1)
    head = k_ref.shape[1]
    rows = q_ref.shape[0]
    block = k_ref.shape[0]

    @pl.when(step == 0)
    def _():
        if last:
            m_ref[...] = m_in[0]
            l_ref[...] = l_in[0]
            a_ref[...] = a_in[0]
        else:
            m_ref[...] = jnp.full_like(m_ref, -1e30)
            l_ref[...] = jnp.zeros_like(l_ref)
            a_ref[...] = jnp.zeros_like(a_ref)

    def update(masked):
        key = k_ref[...]
        value = v_ref[...]
        scale = LOG2E * head ** (-0.5)
        if masked:
            key_pos = step * block + lax.broadcasted_iota(jnp.int32, (rows, block), 1)
            query_pos = row_ref[0] + lax.broadcasted_iota(jnp.int32, (rows, block), 0)
            visible = key_pos <= query_pos
        for g in range(group):
            part = pl.ds(g * rows, rows)
            s = lax.dot_general(
                q_ref[:, g * head : (g + 1) * head],
                key,
                (((1,), (1,)), ((), ())),
                preferred_element_type=jnp.float32,
            )
            if masked:
                s = jnp.where(visible, s, -1e30)
            old = m_ref[part, :]
            new = jnp.maximum(old, jnp.max(s, axis=1, keepdims=True))
            m_ref[part, :] = new
            e = jnp.exp2((s - new[:, :1]) * scale)
            factor = jnp.exp2((old - new) * scale)
            l_ref[part, :] = l_ref[part, :] * factor + jnp.sum(e, axis=1, keepdims=True)
            a_ref[part, :] = a_ref[part, :] * factor + jnp.dot(
                e.astype(jnp.bfloat16), value, preferred_element_type=jnp.float32
            )

    if causal:
        start = step * block

        @pl.when(start + block - 1 <= row_ref[0])
        def _():
            update(False)

        @pl.when((start + block - 1 > row_ref[0]) & (start <= row_ref[0] + rows - 1))
        def _():
            update(True)
    else:
        update(False)

    @pl.when(step == pl.num_programs(1) - 1)
    def _():
        if last:
            for g in range(group):
                part = pl.ds(g * rows, rows)
                out_ref[:, g * head : (g + 1) * head] = (
                    a_ref[part, :] / l_ref[part, :]
                ).astype(out_ref.dtype)
        else:
            m_out[0] = m_ref[...]
            l_out[0] = l_ref[...]
            a_out[0] = a_ref[...]


def attend(query, key_value, first_row, state, head_size):
    rows, width = query.shape
    length = key_value.shape[1]
    kv_local = key_value.shape[2] // head_size
    group = width // head_size // kv_local
    block = 1024
    while length % block:
        block //= 2
    last = state is not None
    high = group * rows
    carry = pl.BlockSpec((1, high, head_size), lambda k, i, r: (k, 0, 0))
    carry_shape = jax.ShapeDtypeStruct((kv_local, high, head_size), jnp.float32)
    wide = pl.BlockSpec((rows, group * head_size), lambda k, i, r: (0, k))
    in_specs = [
        wide,
        pl.BlockSpec((None, block, head_size), lambda k, i, r: (0, i, k)),
        pl.BlockSpec((None, block, head_size), lambda k, i, r: (1, i, k)),
    ] + ([carry] * 3 if last else [])
    operands = (query, key_value, key_value) + (state if last else ())
    return pl.pallas_call(
        functools.partial(attend_kernel, group, last, last),
        out_shape=jax.ShapeDtypeStruct((rows, width), jnp.bfloat16) if last else (carry_shape,) * 3,
        grid_spec=pltpu.PrefetchScalarGridSpec(
            num_scalar_prefetch=1,
            grid=(kv_local, length // block),
            in_specs=in_specs,
            out_specs=wide if last else (carry,) * 3,
            scratch_shapes=[pltpu.VMEM((high, head_size), jnp.float32)] * 3,
        ),
        compiler_params=pltpu.CompilerParams(vmem_limit_bytes=40 * 1024 * 1024),
        cost_estimate=pl.CostEstimate(
            flops=8 * rows * width * length,
            bytes_accessed=4 * length * kv_local * head_size + 4 * rows * width,
            transcendentals=rows * (width // head_size) * length,
        ),
    )(first_row.reshape(1), *operands)


def scatter_kernel(chips, cores, heads, x_ref, o_ref, send_sem, recv_sem, tile, local_sem):
    me = lax.axis_index("ctx")
    h = lax.axis_index("head")
    chip = me // cores
    core = me % cores
    per = chips // heads
    owner_head = chip // per
    slot = h * per + chip % per
    barrier = pltpu.get_barrier_semaphore()
    for d in range(chips):
        there = lax.rem(chip + d, chips) * cores + core
        for e in range(heads):
            if d or e:
                pl.semaphore_signal(
                    barrier,
                    inc=1,
                    device_id=(there, lax.rem(h + e, heads)),
                    device_id_type=pl.DeviceIdType.MESH,
                )
    pl.semaphore_wait(barrier, chips * heads - 1)

    def copy_to(d):
        p = lax.rem(chip + d, chips)
        return pltpu.make_async_remote_copy(
            src_ref=x_ref.at[p],
            dst_ref=o_ref.at[slot],
            send_sem=send_sem.at[d],
            recv_sem=recv_sem.at[slot],
            device_id=(p * cores + core, owner_head),
            device_id_type=pl.DeviceIdType.MESH,
        )

    def receive(s):
        return pltpu.make_async_remote_copy(
            src_ref=x_ref.at[0],
            dst_ref=o_ref.at[s],
            send_sem=send_sem.at[0],
            recv_sem=recv_sem.at[s],
            device_id=(me, lax.rem(h + 1, heads)),
            device_id_type=pl.DeviceIdType.MESH,
        )

    for d in range(1, chips):
        copy_to(d).start()

    @pl.when(owner_head != h)
    def _():
        copy_to(0).start()

    @pl.when(owner_head == h)
    def _():
        into = pltpu.make_async_copy(x_ref.at[chip], tile, local_sem.at[0])
        into.start()
        into.wait()
        out = pltpu.make_async_copy(tile, o_ref.at[slot], local_sem.at[1])
        out.start()
        out.wait()

    for d in range(1, chips):
        copy_to(d).wait_send()

    @pl.when(owner_head != h)
    def _():
        copy_to(0).wait_send()

    for s in range(chips):

        @pl.when(jnp.logical_or(owner_head != h, slot != s))
        def _():
            receive(s).wait_recv()


def scatter_columns(product, chips, cores, heads):
    block = product.shape[1:]
    moved = pl.pallas_call(
        functools.partial(scatter_kernel, chips, cores, heads),
        out_shape=jax.ShapeDtypeStruct(product.shape, product.dtype),
        in_specs=[pl.BlockSpec(memory_space=pl.ANY)],
        out_specs=pl.BlockSpec(memory_space=pl.ANY),
        scratch_shapes=[
            pltpu.SemaphoreType.DMA((chips,)),
            pltpu.SemaphoreType.DMA((chips,)),
            pltpu.VMEM(block, product.dtype),
            pltpu.SemaphoreType.DMA((2,)),
        ],
        compiler_params=pltpu.CompilerParams(collective_id=0, has_side_effects=True),
    )(product)
    return moved.reshape((heads, chips // heads) + block)


def gather_kernel(depth, cores, x_ref, o_ref, send_sem, recv_sem, tile, local_sem):
    me = lax.axis_index("ctx")
    h = lax.axis_index("head")
    chip = me // cores
    core = me % cores
    ring = chip // 2
    side = chip % 2
    pair = ring * 2 + (1 - side)

    def along(d):
        return lax.rem(ring + d, depth)

    barrier = pltpu.get_barrier_semaphore()
    for d in range(1, depth):
        pl.semaphore_signal(
            barrier,
            inc=1,
            device_id=((along(d) * 2 + side) * cores + core, h),
            device_id_type=pl.DeviceIdType.MESH,
        )
    pl.semaphore_signal(
        barrier, inc=1, device_id=(pair * cores + core, h), device_id_type=pl.DeviceIdType.MESH
    )
    pl.semaphore_wait(barrier, depth)

    def send(source, half, origin, target, kind, d):
        return pltpu.make_async_remote_copy(
            src_ref=source,
            dst_ref=o_ref.at[origin, half],
            send_sem=send_sem.at[kind, d],
            recv_sem=recv_sem.at[half, origin],
            device_id=(target * cores + core, h),
            device_id_type=pl.DeviceIdType.MESH,
        )

    def receive(half, origin):
        send(x_ref.at[half], half, origin, pair, 0, 0).wait_recv()

    sent = [send(x_ref.at[0], 0, chip, pair, 0, 0), send(x_ref.at[1], 1, chip, pair, 1, 0)]
    order = [d for pair_of in zip(range(1, depth), range(depth - 1, 0, -1)) for d in pair_of]
    order = list(dict.fromkeys(order))
    for d in order:
        sent.append(send(x_ref.at[1], 1, chip, along(d) * 2 + side, 2, d))
    for d in order:
        sent.append(send(x_ref.at[0], 0, chip, along(d) * 2 + side, 3, d))
    for copy in sent:
        copy.start()
    into = pltpu.make_async_copy(x_ref, tile, local_sem.at[0])
    into.start()
    into.wait()
    out = pltpu.make_async_copy(tile, o_ref.at[chip], local_sem.at[1])
    out.start()

    receive(0, pair)
    for d in order:
        copy = send(o_ref.at[pair, 0], 0, pair, along(d) * 2 + side, 4, d)
        copy.start()
        sent.append(copy)
    for d in order:
        origin = along(d) * 2 + side
        receive(1, origin)
        copy = send(o_ref.at[origin, 1], 1, origin, pair, 1, d)
        copy.start()
        sent.append(copy)
    for d in range(1, depth):
        receive(0, along(d) * 2 + side)
    receive(1, pair)
    for d in range(1, depth):
        receive(0, along(d) * 2 + 1 - side)
        receive(1, along(d) * 2 + 1 - side)
    for copy in sent:
        copy.wait_send()
    out.wait()


def gather_rows(x, chips, cores):
    rows, width = x.shape
    halves = x.reshape(2, rows // 2, width)
    return pl.pallas_call(
        functools.partial(gather_kernel, chips // 2, cores),
        out_shape=jax.ShapeDtypeStruct((chips,) + halves.shape, x.dtype),
        in_specs=[pl.BlockSpec(memory_space=pl.ANY)],
        out_specs=pl.BlockSpec(memory_space=pl.ANY),
        scratch_shapes=[
            pltpu.SemaphoreType.DMA((5, chips // 2)),
            pltpu.SemaphoreType.DMA((2, chips)),
            pltpu.VMEM(halves.shape, x.dtype),
            pltpu.SemaphoreType.DMA((2,)),
        ],
        compiler_params=pltpu.CompilerParams(collective_id=1, has_side_effects=True),
    )(halves).reshape(chips * rows, width)


MESH = pl.DeviceIdType.MESH
EARLY = 4
QUARTERS = 4


def fused_kernel(depth, group, heads, key_block, *refs):
    (cos_ref, sin_ref, q_ref, fresh_ref, hidden_ref, gain_ref, bias_ref, keep_ref, count_ref,
     cached_ref, w_ref, w3_ref, out_ref, packed_ref,
     qrot, qall, frot, kc, kf, s_ref, av, st, wv, w3, acc_ref, cst, crecv, rows_ref, gains,
     kvs, kvr, kys, kcs, loc, qs, qr, ws, wr, wos, wor, wfs, wfr,
     xs, xr, us, ds, ys, zr, yr, cs, cr, ls, lr, gs, gr) = refs
    rows = q_ref.shape[0]
    head_size = kc.shape[2]
    quarter = rows // QUARTERS
    half = quarter // heads
    cached_rows = cached_ref.shape[1]
    chips = depth * 2
    per = chips // heads
    me = lax.axis_index("ctx")
    h = lax.axis_index("head")
    chip = me // 2
    c = me % 2
    z = chip // 2
    y = chip % 2
    pieces = ws.shape[0]
    piece = w_ref.shape[0] // pieces
    width = w_ref.shape[1]
    last = QUARTERS - 1

    def ctx(zz, yy, cc):
        return (zz * 2 + yy) * 2 + cc

    def remote(src, dst, ssem, rsem, zz, yy, cc, hh):
        return pltpu.make_async_remote_copy(
            src_ref=src, dst_ref=dst, send_sem=ssem, recv_sem=rsem,
            device_id=(ctx(zz, yy, cc), hh), device_id_type=MESH,
        )

    def landed(where, rsem):
        remote(where, where, ls.at[0], rsem, z, 1 - y, c, h).wait_recv()

    barrier = pltpu.get_barrier_semaphore()
    for d in range(chips):
        for e in range(heads):
            if d or e:
                pl.semaphore_signal(
                    barrier, inc=1,
                    device_id=(lax.rem(chip + d, chips) * 2 + c, lax.rem(h + e, heads)),
                    device_id_type=MESH,
                )
    pl.semaphore_signal(barrier, inc=1, device_id=(ctx(z, y, 1 - c), h), device_id_type=MESH)

    def lanes(index):
        return pl.ds(pl.multiple_of(index * head_size, head_size), head_size)

    def slot(kind, zz, yy, cc):
        where = ctx(zz, yy, cc)
        if kind == 0:
            return kc.at[:, pl.ds(pl.multiple_of(where * cached_rows, cached_rows), cached_rows), :]
        return kf.at[:, pl.ds(pl.multiple_of(where * rows, rows), rows), :]

    own_c = pltpu.make_async_copy(cached_ref.at[:, :, lanes(z)], slot(0, z, y, c), loc.at[0])
    own_c.start()
    own_w = pltpu.make_async_copy(w_ref, wv.at[h, c], loc.at[1])
    own_w.start()

    cosine = cos_ref[...]
    sine = sin_ref[...]

    def rotate(x):
        x = x.astype(jnp.float32)
        return x * cosine + pltpu.roll(x, head_size // 2, 1) * sine

    for g in range(depth):
        part = slice(g * head_size, (g + 1) * head_size)
        frot[g, 0] = rotate(fresh_ref[0, :, part]).astype(jnp.bfloat16)
        frot[g, 1] = fresh_ref[1, :, part]
    own_f = pltpu.make_async_copy(frot.at[z], slot(1, z, y, c), loc.at[2])
    own_f.start()

    def kv_send(d, kind):
        to = lax.rem(z + d, depth)
        src = cached_ref.at[:, :, lanes(to)] if kind == 0 else frot.at[to]
        return remote(
            src, slot(kind, z, y, c), kvs.at[d, kind], kvr.at[kind, ctx(z, y, c)], to, y, c, h
        )

    def kv_pair(zz, kind):
        where = slot(kind, zz, y, c)
        return remote(where, where, kys.at[zz, kind], kvr.at[kind, ctx(zz, y, c)], z, 1 - y, c, h)

    def kv_core(zz, yy, kind):
        where = slot(kind, zz, yy, c)
        return remote(
            where, where, kcs.at[zz * 2 + yy, kind], kvr.at[kind, ctx(zz, yy, c)], z, y, 1 - c, h
        )

    def kv_landed(zz, yy, cc, kind):
        landed(slot(kind, zz, yy, cc), kvr.at[kind, ctx(zz, yy, cc)])

    def q_send(i, d):
        to = lax.rem(z + d, depth)
        return remote(qrot.at[to, i], qall.at[i, z], qs.at[i, d], qr.at[i, z], to, y, c, h)

    def w_part(k):
        return pl.ds(pl.multiple_of(k * piece, piece), piece)

    def w_send(k):
        return remote(
            w_ref.at[w_part(k), :], wv.at[h, c, w_part(k), :], ws.at[k], wr.at[k], z, y, c, 1 - h
        )

    def w_forward(k):
        where = wv.at[1 - h, c, w_part(k), :]
        return remote(where, where, wfs.at[k], wfr.at[k], z, y, 1 - c, h)

    def forward(k, carry):
        landed(wv.at[1 - h, c, w_part(k), :], wr.at[k])
        w_forward(k).start()
        return carry

    own_w_core = remote(w_ref, wv.at[h, c], wos.at[0], wor.at[0], z, y, 1 - c, h)
    gain_send = remote(gain_ref, gains.at[h], gs.at[0], gr.at[0], z, y, c, 1 - h)

    pl.semaphore_wait(barrier, chips * heads)
    for kind in range(2):
        for d in range(1, depth):
            kv_send(d, kind).start()
    for k in range(EARLY):
        w_send(k).start()
    own_c.wait()
    own_f.wait()
    for kind in range(2):
        kv_pair(z, kind).start()
        kv_core(z, y, kind).start()

    for j in range(depth * group):
        x = rotate(q_ref[:, j * head_size : (j + 1) * head_size]).astype(jnp.bfloat16)
        for i in range(QUARTERS):
            qrot[j // group, i, j % group] = x[i * quarter : (i + 1) * quarter]
    for i in range(QUARTERS):
        qall[i, z] = qrot[z, i]

    for s in range(1, depth):
        for sign in (-1, 1):
            zz = z + sign * s

            @pl.when((zz >= 0) & (zz < depth))
            def _():
                for kind in range(2):
                    kv_landed(zz, y, c, kind)
                    kv_pair(zz, kind).start()
                    kv_core(zz, y, kind).start()

        if s == 1:
            for i in range(QUARTERS):
                for d in range(1, depth):
                    q_send(i, d).start()

    for zz in range(depth):
        for kind in range(2):
            kv_landed(zz, 1 - y, c, kind)
            kv_core(zz, 1 - y, kind).start()
    gain_send.start()
    for zz in range(depth):
        for yy in range(2):
            for kind in range(2):
                kv_landed(zz, yy, 1 - c, kind)
    own_w_core.start()
    own_w3 = pltpu.make_async_copy(w3_ref, w3, loc.at[3])
    own_w3.start()

    def side(w):
        return lax.rem(h + w, 2)

    def x_send(e):
        return remote(st.at[e], av.at[e, h, z, y], xs.at[e], xr.at[e], z, y, c, 1 - h)

    def unit(e, w, zz, yy):
        return av.at[e, side(w), zz, yy]

    def up(e, w, zz):
        where = unit(e, w, zz, y)
        return remote(where, where, us.at[e, w, zz], zr.at[e, w, zz], z + 1, y, c, h)

    def down(e, w, zz):
        where = unit(e, w, zz, y)
        return remote(where, where, ds.at[e, w, zz], zr.at[e, w, zz], z - 1, y, c, h)

    def across(e, w, zz):
        where = unit(e, w, zz, y)
        return remote(where, where, ys.at[e, w, zz], yr.at[e, w, zz], z, 1 - y, c, h)

    def own_out(e, w):
        if w:
            landed(unit(e, w, z, y), xr.at[e])

        @pl.when(z + 1 < depth)
        def _():
            up(e, w, z).start()

        @pl.when(z >= 1)
        def _():
            down(e, w, z).start()

        across(e, w, z).start()

    def hop(e, w, s):
        @pl.when(z >= s)
        def _():
            landed(unit(e, w, z - s, y), zr.at[e, w, z - s])

            @pl.when(z + 1 < depth)
            def _():
                up(e, w, z - s).start()

            across(e, w, z - s).start()

        @pl.when(z + s < depth)
        def _():
            landed(unit(e, w, z + s, y), zr.at[e, w, z + s])

            @pl.when(z >= 1)
            def _():
                down(e, w, z + s).start()

            across(e, w, z + s).start()

    scale = LOG2E * head_size ** (-0.5)
    both = group * quarter
    lane_groups = key_block // head_size
    cached_blocks = kc.shape[1] // key_block

    def attend(i, zp):
        q = qall[i, zp].reshape(both, head_size)
        start = ctx(zp, y, c) * rows + i * quarter
        fresh_blocks = (start + quarter + key_block - 1) // key_block

        def scores(keys):
            return lax.dot_general(
                q, keys, (((1,), (1,)), ((), ())), preferred_element_type=jnp.float32
            )

        def widen(s, top):
            for u in range(lane_groups):
                top = jnp.maximum(top, s[:, u * head_size : (u + 1) * head_size])
            return top

        top = jnp.full((both, head_size), -1e30, jnp.float32)
        for b in range(cached_blocks):
            s = scores(kc[0, b * key_block : (b + 1) * key_block, :])
            s_ref[b] = s
            top = widen(s, top)

        def fresh_scores(b, top):
            keys = kf[0, pl.ds(pl.multiple_of(b * key_block, key_block), key_block), :]
            s = scores(keys)
            key_pos = b * key_block + lax.broadcasted_iota(jnp.int32, (quarter, key_block), 1)
            query_pos = start + lax.broadcasted_iota(jnp.int32, (quarter, key_block), 0)
            visible = key_pos <= query_pos
            s = jnp.where(jnp.concatenate([visible] * group, axis=0), s, -1e30)
            s_ref[cached_blocks + b] = s
            return widen(s, top)

        top = lax.fori_loop(0, fresh_blocks, fresh_scores, top)
        peak = jnp.max(top, axis=1, keepdims=True)

        def weigh(s, values, total, summed):
            e = jnp.exp2((s - peak) * scale)
            for u in range(lane_groups):
                total = total + e[:, u * head_size : (u + 1) * head_size]
            summed = summed + jnp.dot(
                e.astype(jnp.bfloat16), values, preferred_element_type=jnp.float32
            )
            return total, summed

        total = jnp.zeros((both, head_size), jnp.float32)
        summed = jnp.zeros((both, head_size), jnp.float32)
        for b in range(cached_blocks):
            total, summed = weigh(
                s_ref[b], kc[1, b * key_block : (b + 1) * key_block, :], total, summed
            )

        def fresh_weigh(b, carry):
            values = kf[1, pl.ds(pl.multiple_of(b * key_block, key_block), key_block), :]
            return weigh(s_ref[cached_blocks + b], values, *carry)

        total, summed = lax.fori_loop(0, fresh_blocks, fresh_weigh, (total, summed))
        out = (summed / jnp.sum(total, axis=1, keepdims=True)).astype(jnp.bfloat16)
        where = pl.ds(pl.multiple_of(zp * half, half), half)
        for a in range(group):
            upper = out[a * quarter : a * quarter + half]
            lower = out[a * quarter + half : (a + 1) * quarter]
            part = slice(a * head_size, (a + 1) * head_size)
            av[i, h, z, y, where, part] = jnp.where(h == 0, upper, lower)
            st[i, where, part] = jnp.where(h == 0, lower, upper)

    def step(t, carry):
        i = t // depth
        p = t % depth
        zp = lax.rem(z + p, depth)

        @pl.when(p != 0)
        def _():
            landed(qall.at[i, zp], qr.at[i, zp])

        attend(i, zp)

        @pl.when(p >= 1)
        def _():
            w_send(EARLY + (depth - 1) * i + p - 1).start()

        @pl.when((p == 0) & (i >= 1))
        def _():
            x_send(i - 1).start()
            own_out(i - 1, 0)

        @pl.when((p == 0) & (i >= 2))
        def _():
            hop(i - 2, 0, 2)

        @pl.when((p == 1) & (i >= 1))
        def _():
            own_out(i - 1, 1)
            low = jnp.where(i == 1, 0, EARLY + (depth - 1) * (i - 2))
            lax.fori_loop(low, EARLY + (depth - 1) * (i - 1), forward, 0)

        @pl.when((p == 1) & (i >= 2))
        def _():
            hop(i - 2, 1, 2)

        for w in range(2):
            @pl.when((p == depth - 2 + w) & (i >= 1))
            def _():
                hop(i - 1, w, 1)

            @pl.when((p == depth - 2 + w) & (i >= 2))
            def _():
                for s in range(3, depth):
                    hop(i - 2, w, s)

        return carry

    lax.fori_loop(0, QUARTERS * depth, step, 0)

    owner = chip // per
    place = chip % per
    span = av.shape[5]

    def tile_send(e, zp, yy):
        return remote(
            cst.at[e, yy, zp], crecv.at[e, h, place], cs.at[e, yy, zp], cr.at[e, h, place],
            zp, yy, c, owner,
        )

    def is_self(zp, yy):
        return (z == zp) & (y == yy) & (owner == h)

    def project(e):
        for w in range(2):
            for zz in range(depth):
                landed(unit(e, w, zz, 1 - y), yr.at[e, w, zz])
        acc_ref[...] = jnp.zeros_like(acc_ref)

        def term(k, carry):
            xx = k // depth
            zz = k % depth
            left = av[e, xx, zz].reshape(2 * depth * half, span)
            for cc in range(2):
                acc_ref[:, cc * width : (cc + 1) * width] += jnp.dot(
                    left,
                    wv[xx, cc, pl.ds(pl.multiple_of(zz * span, span), span), :],
                    preferred_element_type=jnp.float32,
                )
            return carry

        lax.fori_loop(0, heads * depth, term, 0)
        for yy in range(2):
            for zp in range(depth):
                low = (yy * depth + zp) * half
                cst[e, yy, zp] = acc_ref[low : low + half, :].astype(jnp.bfloat16)
        for yy in range(2):
            for zp in range(depth):
                @pl.when(is_self(zp, yy))
                def _():
                    crecv[e, h, place] = cst[e, yy, zp]

                @pl.when(jnp.logical_not(is_self(zp, yy)))
                def _():
                    tile_send(e, zp, yy).start()

    def rows_send(e):
        return remote(rows_ref.at[h, e], rows_ref.at[h, e], ls.at[e], lr.at[e], z, y, c, 1 - h)

    def finish(e):
        for xx in range(heads):
            for s in range(per):
                @pl.when(jnp.logical_not((h * per + s == chip) & (h == xx)))
                def _():
                    landed(crecv.at[e, xx, s], cr.at[e, xx, s])

                rows_of = slice(e * quarter + xx * half, e * quarter + (xx + 1) * half)
                columns = slice(s * 2 * width, (s + 1) * 2 * width)
                done = (
                    hidden_ref[rows_of, columns].astype(jnp.float32)
                    + crecv[e, xx, s].astype(jnp.float32)
                ).astype(jnp.bfloat16)
                out_ref[rows_of, columns] = done
                rows_ref[h, e, xx * half : (xx + 1) * half, columns] = done
        rows_send(e).start()

    x_send(last).start()
    own_out(last, 0)
    hop(last - 1, 0, 2)
    own_out(last, 1)
    hop(last - 1, 1, 2)
    for w in range(2):
        hop(last, w, 1)
        for s in range(3, depth):
            hop(last - 1, w, s)
    lax.fori_loop(EARLY + (depth - 1) * (last - 1), pieces, forward, 0)
    for s in range(2, depth):
        for w in range(2):
            hop(last, w, s)
    own_w.wait()
    landed(wv.at[h, 1 - c], wor.at[0])

    def forwarded(k, carry):
        landed(wv.at[1 - h, 1 - c, w_part(k), :], wfr.at[k])
        return carry

    lax.fori_loop(0, pieces, forwarded, 0)
    project(0)
    for e in range(1, QUARTERS):
        project(e)
        finish(e - 1)
    own_w3.wait()
    gains[h] = gain_ref[...]
    landed(gains.at[1 - h], gr.at[0])
    finish(last)

    for e in range(QUARTERS):
        landed(rows_ref.at[1 - h, e], lr.at[e])
    model = rows_ref.shape[3]
    squares = jnp.zeros((rows, head_size), jnp.float32)
    for xx in range(heads):
        for k in range(model // head_size):
            part = slice(k * head_size, (k + 1) * head_size)
            x = rows_ref[xx, :, :, part].reshape(rows, head_size).astype(jnp.float32)
            squares = squares + x * x
    level = lax.rsqrt(jnp.sum(squares, axis=1, keepdims=True) / (heads * model) + 1e-06)
    acc_ref[...] = jnp.zeros_like(acc_ref)
    for xx in range(heads):
        for k in range(model // span):
            part = slice(k * span, (k + 1) * span)
            x = rows_ref[xx, :, :, part].reshape(rows, span).astype(jnp.float32)
            normed = (x * level * gains[xx, :, part]).astype(jnp.bfloat16)
            low = xx * model + k * span
            acc_ref[...] += jnp.dot(
                normed, w3[low : low + span, :], preferred_element_type=jnp.float32
            )
    chosen = keep_ref[...] == lax.broadcasted_iota(jnp.int32, (rows, rows), 1)
    filled = lax.broadcasted_iota(jnp.int32, (rows, rows), 0) < count_ref[...]
    pick = jnp.where(chosen & filled, 1.0, 0.0).astype(jnp.bfloat16)
    for g in range(2 * depth):
        part = slice(g * head_size, (g + 1) * head_size)
        x = acc_ref[:, part] + bias_ref[:, part]
        if g % 2 == 0:
            x = rotate(x)
        packed_ref[:, part] = jnp.dot(
            pick, x.astype(jnp.bfloat16), preferred_element_type=jnp.float32
        ).astype(jnp.bfloat16)

    for d in range(1, depth):
        for kind in range(2):
            kv_send(d, kind).wait_send()
        for i in range(QUARTERS):
            q_send(i, d).wait_send()
    for zz in range(depth):
        for kind in range(2):
            kv_pair(zz, kind).wait_send()
            for yy in range(2):
                kv_core(zz, yy, kind).wait_send()
    own_w_core.wait_send()
    gain_send.wait_send()

    def w_sent(k, carry):
        w_send(k).wait_send()
        w_forward(k).wait_send()
        return carry

    lax.fori_loop(0, pieces, w_sent, 0)

    def sent(e, carry):
        x_send(e).wait_send()
        rows_send(e).wait_send()
        for zz in range(depth):
            for w in range(2):
                across(e, w, zz).wait_send()

                @pl.when((zz <= z) & (z + 1 < depth))
                def _():
                    up(e, w, zz).wait_send()

                @pl.when((zz >= z) & (z >= 1))
                def _():
                    down(e, w, zz).wait_send()

            for yy in range(2):
                @pl.when(jnp.logical_not(is_self(zz, yy)))
                def _():
                    tile_send(e, zz, yy).wait_send()

        return carry

    lax.fori_loop(0, QUARTERS, sent, 0)


def fused(tables_of, query, fresh, hidden, gain, bias, keep, count, cached, weight, weight3,
          depth, heads):
    rows, wide = query.shape
    head_size = HEAD_DIMENSION
    group = wide // head_size // depth
    contexts = depth * 4
    quarter = rows // QUARTERS
    half = quarter // heads
    key_block = 512
    cached_total = contexts * cached.shape[1]
    fresh_total = contexts * rows
    while cached_total % key_block or fresh_total % key_block:
        key_block //= 2
    pieces = EARLY + (depth - 1) * QUARTERS
    per = depth * 2 // heads
    model = hidden.shape[1]
    out3 = weight3.shape[1]
    dma = pltpu.SemaphoreType.DMA
    bf16 = jnp.bfloat16
    vmem = pltpu.VMEM
    whole = pl.BlockSpec(memory_space=pltpu.VMEM)
    far = pl.BlockSpec(memory_space=pl.ANY)
    links = dma((QUARTERS, 2, depth))
    return pl.pallas_call(
        functools.partial(fused_kernel, depth, group, heads, key_block),
        out_shape=(
            jax.ShapeDtypeStruct(hidden.shape, bf16),
            jax.ShapeDtypeStruct((rows, out3), bf16),
        ),
        in_specs=[whole] * 9 + [far] * 3,
        out_specs=(whole, whole),
        scratch_shapes=[
            vmem((depth, QUARTERS, group, quarter, head_size), bf16),
            vmem((QUARTERS, depth, group, quarter, head_size), bf16),
            vmem((depth, 2, rows, head_size), bf16),
            vmem((2, cached_total, head_size), bf16),
            vmem((2, fresh_total, head_size), bf16),
            vmem(
                ((cached_total + fresh_total) // key_block, group * quarter, key_block),
                jnp.float32,
            ),
            vmem((QUARTERS, heads, depth, 2, depth * half, group * head_size), bf16),
            vmem((QUARTERS, depth * half, group * head_size), bf16),
            vmem((heads, 2) + weight.shape, bf16),
            vmem(weight3.shape, bf16),
            vmem((rows, 2 * weight.shape[1]), jnp.float32),
            vmem((QUARTERS, 2, depth, half, 2 * weight.shape[1]), bf16),
            vmem((QUARTERS, heads, per, half, 2 * weight.shape[1]), bf16),
            vmem((heads, QUARTERS, quarter, model), bf16),
            vmem((heads, 1, model), jnp.float32),
            dma((depth, 2)), dma((2, contexts)), dma((depth, 2)), dma((depth * 2, 2)),
            dma((4,)), dma((QUARTERS, depth)), dma((QUARTERS, depth)),
            dma((pieces,)), dma((pieces,)), dma((1,)), dma((1,)), dma((pieces,)), dma((pieces,)),
            dma((QUARTERS,)), dma((QUARTERS,)),
            links, links, links, links, links,
            dma((QUARTERS, 2, depth)), dma((QUARTERS, heads, per)),
            dma((QUARTERS,)), dma((QUARTERS,)), dma((1,)), dma((1,)),
        ],
        compiler_params=pltpu.CompilerParams(
            collective_id=2, has_side_effects=True, vmem_limit_bytes=67043328
        ),
    )(*tables_of, query, fresh, hidden, gain.reshape(1, model), bias.reshape(1, out3),
      keep.reshape(rows, 1), count.reshape(1, 1), cached, weight, weight3)


def exchange(x, axis_name, size):
    return lax.ppermute(x, axis_name, [(i, i ^ 1) for i in range(size)])


def local(
    contexts,
    heads,
    hidden,
    query,
    fresh_key_value,
    cached_key_value,
    positions,
    out_weight,
    norm_gain,
    layer3_key_value_weight,
    layer3_key_value_bias,
    keep_index,
    keep_count,
):
    new_rows = hidden.shape[0]
    head_size = HEAD_DIMENSION
    kv_local = fresh_key_value.shape[2] // head_size
    q_local = query.shape[1] // head_size
    cores = 2
    chips = contexts // cores
    me = lax.axis_index("ctx")
    core = me % cores
    head = lax.axis_index("head")
    cosine_table, sine_table = tables(positions, head_size)
    if heads == 2 and kv_local * 2 == chips and kv_local >= 4 and q_local == 8 * kv_local:
        return fused(
            (
                jnp.concatenate([cosine_table, cosine_table], axis=1),
                jnp.concatenate([-sine_table, sine_table], axis=1),
            ),
            query,
            fresh_key_value,
            hidden,
            norm_gain,
            layer3_key_value_bias,
            keep_index,
            keep_count,
            cached_key_value,
            out_weight,
            layer3_key_value_weight,
            kv_local,
            heads,
        )
    rotary_query_rows = apply_rotary(
        query.astype(jnp.float32).reshape(new_rows, q_local, head_size), cosine_table, sine_table
    ).astype(jnp.bfloat16).reshape(new_rows, q_local * head_size)
    rotary_key_rows = apply_rotary(
        fresh_key_value[0].astype(jnp.float32).reshape(new_rows, kv_local, head_size),
        cosine_table,
        sine_table,
    ).astype(jnp.bfloat16)
    recent = jnp.stack(
        [rotary_key_rows.reshape(new_rows, kv_local * head_size), fresh_key_value[1]]
    )
    if heads == 2:
        other_gain = exchange(norm_gain, "head", heads)
        whole_gain = jnp.concatenate(
            [jnp.where(head == 0, norm_gain, other_gain), jnp.where(head == 0, other_gain, norm_gain)]
        )
    else:
        whole_gain = lax.all_gather(norm_gain, "head", axis=0, tiled=True)
    other_weight = exchange(out_weight, "ctx", contexts)
    first_row = me * new_rows
    cached_all = lax.all_gather(cached_key_value, "ctx", axis=1, tiled=True)
    recent_all = lax.all_gather(recent, "ctx", axis=1, tiled=True)
    state = attend(rotary_query_rows, cached_all, first_row, None, head_size)
    attn = attend(rotary_query_rows, recent_all, first_row, tuple(state), head_size)
    outputs = gather_rows(attn, chips, cores)
    own = jnp.dot(outputs, out_weight, preferred_element_type=jnp.float32).astype(jnp.bfloat16)
    other = jnp.dot(outputs, other_weight, preferred_element_type=jnp.float32).astype(jnp.bfloat16)
    product = jnp.concatenate(
        [jnp.where(core == 0, own, other), jnp.where(core == 0, other, own)], axis=1
    ).reshape(chips, new_rows, -1)
    parts = scatter_columns(product, chips, cores, heads)
    head_summed = jnp.sum(parts.astype(jnp.float32), axis=0)
    head_summed = head_summed.transpose(1, 0, 2).reshape(hidden.shape)
    layer2_out = (hidden.astype(jnp.float32) + head_summed).astype(jnp.bfloat16)
    if heads == 2:
        other_out = exchange(layer2_out, "head", heads)
        whole_out = jnp.concatenate(
            [
                jnp.where(head == 0, layer2_out, other_out),
                jnp.where(head == 0, other_out, layer2_out),
            ],
            axis=1,
        )
    else:
        whole_out = lax.all_gather(layer2_out, "head", axis=1, tiled=True)
    widened = whole_out.astype(jnp.float32)
    squares = jnp.sum(widened * widened, axis=1)
    level = lax.rsqrt(squares / widened.shape[1] + 1e-06)[:, None]
    full_rows = (widened * level * whole_gain).astype(jnp.bfloat16)
    full_rows = lax.optimization_barrier(full_rows)
    layer_three_key_value = (
        jnp.dot(full_rows, layer3_key_value_weight, preferred_element_type=jnp.float32)
        + layer3_key_value_bias
    ).reshape(new_rows, kv_local, 2, head_size)
    layer_three_keys = apply_rotary(layer_three_key_value[:, :, 0], cosine_table, sine_table)
    layer_three_key_value = (
        jnp.stack([layer_three_keys, layer_three_key_value[:, :, 1]], axis=2)
        .reshape(new_rows, 2 * kv_local * head_size)
        .astype(jnp.bfloat16)
    )
    selected_rows = jnp.take(layer_three_key_value, keep_index, axis=0)
    block_occupied = jnp.arange(new_rows) < keep_count[0]
    layer3_packed_key_value = jnp.where(
        block_occupied[:, None], selected_rows, jnp.zeros_like(selected_rows)
    )
    return (layer2_out, layer3_packed_key_value)


def solution(mesh):
    placed = (
        P("ctx", "head"),
        P("ctx", "head"),
        P(None, "ctx", "head"),
        P(None, "ctx", "head"),
        P(None, "ctx"),
        P("head", "ctx"),
        P("head"),
        P(None, "head"),
        P("head"),
        P("ctx"),
        P("ctx"),
    )
    return jax.shard_map(
        functools.partial(local, mesh.shape["ctx"], mesh.shape["head"]),
        mesh=mesh,
        in_specs=placed,
        out_specs=(P("ctx", "head"), P("ctx", "head")),
        check_vma=False,
    )
```
